32 devices in a mesh: dp: 4 (over y, z), tp: 8 (over x, core).
Axes of the slice: x: 4, y: 2, z: 2, core: 2. Of those that a mesh axis runs over, the one named last changes fastest.
The devices are a block of a 4x4x8 slice.
Arguments:
- tokens: bfloat16 [4, 2048, 2048], P('dp', 'tp'), parts along dimension 0
- doc_ids: int32 [4, 2048], P('dp', 'tp'), parts along dimension 0
- norm1_gain: float32 [2, 2048], replicated
- norm1_shift: float32 [2, 2048], replicated
- qkv_weight: bfloat16 [2, 2048, 3, 32, 64], P(None, None, None, 'tp')
- out_weight: bfloat16 [2, 32, 64, 2048], P(None, 'tp')
- out_bias: float32 [2, 2048], replicated
- norm2_gain: float32 [2, 2048], replicated
- norm2_shift: float32 [2, 2048], replicated
- up_weight: bfloat16 [2, 2048, 8192], P(None, None, 'tp')
- up_bias: float32 [2, 8192], P(None, 'tp')
- down_weight: bfloat16 [2, 8192, 2048], P(None, 'tp')
- down_bias: float32 [2, 2048], replicated
Outputs:
- output: bfloat16 [4, 2048, 2048], P('dp', 'tp'), parts along dimension 0
There are 4 independent parts. The reference program is written for one: setup_inputs(seed, part) draws one part's arguments, and reference() takes and returns one part's arrays. A program takes and returns all parts, laid end to end along the dimension named above; an argument that names none is the same for every part.
All inputs are finite; a program needn't handle non-finite values.
Results may differ from the reference program's by a relative error of at most 0.0119882.
Values are sent between devices in bfloat16 or wider.
A program may use at most 768 MiB of HBM per device.

```python
import jax
import jax.numpy as jnp
from jax import lax

BATCH = 1
SEQ_LEN = 2048
D_MODEL = 2048
N_HEADS = 32
HEAD_DIM = 64
FF_DIM = 8192
GROUPS = 8
LAYERS = 2
DOC_CUTS = 3
QUERY_BLOCK = 256


def setup_inputs(seed: int = 0, part: int = 0) -> dict:
    root_key = jax.random.key(seed)
    keys_all = jax.random.split(root_key, 12)
    part_key = jax.random.fold_in(keys_all[0], part)
    tok_key, scale_key, cut_key = jax.random.split(part_key, 3)
    base_tok = jax.random.normal(tok_key, (BATCH, SEQ_LEN, D_MODEL), jnp.float32)
    row_scale = jnp.exp(0.5 * jax.random.normal(scale_key, (BATCH, SEQ_LEN, 1), jnp.float32))
    tokens = (base_tok * row_scale).astype(jnp.bfloat16)
    cut_pos = jax.random.randint(cut_key, (BATCH, 1, DOC_CUTS), 1, SEQ_LEN, dtype=jnp.int32)
    positions = jnp.arange(SEQ_LEN, dtype=jnp.int32)[None, :, None]
    doc_ids = jnp.sum((positions >= cut_pos).astype(jnp.int32), axis=-1, dtype=jnp.int32)
    d_scale = D_MODEL ** -0.5
    f_scale = FF_DIM ** -0.5
    qkv_mult = jnp.array([1.4142135, 1.4142135, 1.0], jnp.float32)[None, None, :, None, None]
    vec_shape = (LAYERS, D_MODEL)
    qkv_weight = jax.random.normal(keys_all[1], (LAYERS, D_MODEL, 3, N_HEADS, HEAD_DIM), jnp.float32) * qkv_mult * d_scale
    out_weight = jax.random.normal(keys_all[2], (LAYERS, N_HEADS, HEAD_DIM, D_MODEL), jnp.float32) * (1.5 * d_scale)
    up_weight = jax.random.normal(keys_all[3], (LAYERS, D_MODEL, FF_DIM), jnp.float32) * d_scale
    down_weight = jax.random.normal(keys_all[4], (LAYERS, FF_DIM, D_MODEL), jnp.float32) * f_scale
    return {
        "tokens": tokens,
        "doc_ids": doc_ids,
        "norm1_gain": 1.0 + 0.2 * jax.random.normal(keys_all[5], vec_shape, jnp.float32),
        "norm1_shift": 0.2 * jax.random.normal(keys_all[6], vec_shape, jnp.float32),
        "qkv_weight": qkv_weight.astype(jnp.bfloat16),
        "out_weight": out_weight.astype(jnp.bfloat16),
        "out_bias": 0.3 * jax.random.normal(keys_all[7], vec_shape, jnp.float32),
        "norm2_gain": 1.0 + 0.2 * jax.random.normal(keys_all[8], vec_shape, jnp.float32),
        "norm2_shift": 0.2 * jax.random.normal(keys_all[9], vec_shape, jnp.float32),
        "up_weight": up_weight.astype(jnp.bfloat16),
        "up_bias": 0.5 * jax.random.normal(keys_all[10], (LAYERS, FF_DIM), jnp.float32),
        "down_weight": down_weight.astype(jnp.bfloat16),
        "down_bias": 0.3 * jax.random.normal(keys_all[11], vec_shape, jnp.float32),
    }


def layer_norm(residual, gain_vec, shift_vec):
    mean_val = jnp.mean(residual, axis=-1, keepdims=True)
    centered = residual - mean_val
    variance = jnp.mean(centered * centered, axis=-1, keepdims=True)
    return (centered * lax.rsqrt(variance + 1e-5) * gain_vec + shift_vec).astype(jnp.bfloat16)


def attend_sequence(qkv_seq, ids_seq):
    n_blocks = SEQ_LEN // QUERY_BLOCK
    keys32 = qkv_seq[:, 1].astype(jnp.float32)
    values32 = qkv_seq[:, 2].astype(jnp.float32)
    q_blocks = qkv_seq[:, 0].reshape(n_blocks, QUERY_BLOCK, N_HEADS, HEAD_DIM)
    id_blocks = ids_seq.reshape(n_blocks, QUERY_BLOCK)
    starts = jnp.arange(n_blocks, dtype=jnp.int32) * QUERY_BLOCK
    key_pos = jnp.arange(SEQ_LEN, dtype=jnp.int32)

    def one_block(block_in):
        q_blk, id_blk, start_row = block_in
        scores = jnp.einsum("qhe,khe->hqk", q_blk.astype(jnp.float32), keys32) * (HEAD_DIM ** -0.5)
        query_pos = start_row + jnp.arange(QUERY_BLOCK, dtype=jnp.int32)
        allowed = (key_pos[None, :] <= query_pos[:, None]) & (ids_seq[None, :] == id_blk[:, None])
        scores = jnp.where(allowed[None], scores, -1e30)
        probs_blk = jax.nn.softmax(scores, axis=-1).astype(jnp.bfloat16)
        return jnp.einsum("hqk,khe->qhe", probs_blk.astype(jnp.float32), values32).astype(jnp.bfloat16)

    return lax.map(one_block, (q_blocks, id_blocks, starts)).reshape(SEQ_LEN, N_HEADS, HEAD_DIM)


def grouped_sum(activations, weight):
    def add_group(running, group_in):
        act_g, weight_g = group_in
        part_out = jnp.dot(act_g, weight_g, preferred_element_type=jnp.float32).astype(jnp.bfloat16)
        return running + part_out.astype(jnp.float32), None
    zero_acc = jnp.zeros((activations.shape[1], weight.shape[2]), jnp.float32)
    total, unused = lax.scan(add_group, zero_acc, (activations, weight))
    return total


def run_sequence(tok_seq, ids_seq, layer_params):
    head_group = N_HEADS // GROUPS
    ff_group = FF_DIM // GROUPS

    def one_layer(residual, params):
        n1_gain, n1_shift, w_qkv, w_out, b_out, n2_gain, n2_shift, w_up, b_up, w_down, b_down = params
        normed = layer_norm(residual, n1_gain, n1_shift)
        qkv_seq = jnp.dot(normed, w_qkv.reshape(D_MODEL, 3 * N_HEADS * HEAD_DIM), preferred_element_type=jnp.float32).astype(jnp.bfloat16)
        attn_out = attend_sequence(qkv_seq.reshape(SEQ_LEN, 3, N_HEADS, HEAD_DIM), ids_seq)
        attn_groups = jnp.moveaxis(attn_out.reshape(SEQ_LEN, GROUPS, head_group * HEAD_DIM), 1, 0)
        attn_sum = grouped_sum(attn_groups, w_out.reshape(GROUPS, head_group * HEAD_DIM, D_MODEL))
        residual = residual + (attn_sum + b_out)
        normed2 = layer_norm(residual, n2_gain, n2_shift)
        pre_act = jnp.dot(normed2, w_up, preferred_element_type=jnp.float32) + b_up
        hidden = jax.nn.gelu(pre_act, approximate=True).astype(jnp.bfloat16)
        hid_groups = jnp.moveaxis(hidden.reshape(SEQ_LEN, GROUPS, ff_group), 1, 0)
        mlp_sum = grouped_sum(hid_groups, w_down.reshape(GROUPS, ff_group, D_MODEL))
        residual = residual + (mlp_sum + b_down)
        return residual, None

    resid_end, unused = lax.scan(one_layer, tok_seq.astype(jnp.float32), layer_params)
    return resid_end.astype(jnp.bfloat16)


def reference(tokens, doc_ids, norm1_gain, norm1_shift, qkv_weight, out_weight, out_bias, norm2_gain, norm2_shift, up_weight, up_bias, down_weight, down_bias):
    layer_params = (norm1_gain, norm1_shift, qkv_weight, out_weight, out_bias, norm2_gain, norm2_shift, up_weight, up_bias, down_weight, down_bias)
    return lax.map(lambda seq_in: run_sequence(seq_in[0], seq_in[1], layer_params), (tokens, doc_ids))
```

```python
import jax
import jax.numpy as jnp
from jax import lax
from jax.experimental import pallas as pl
from jax.experimental.pallas import tpu as pltpu
from jax.sharding import PartitionSpec as P

F32 = jnp.float32
BF16 = jnp.bfloat16
QB = 256
LOG2E = 1.4426950408889634


def layer_norm(residual, gain_vec, shift_vec):
    mean_val = jnp.mean(residual, axis=-1, keepdims=True)
    centered = residual - mean_val
    variance = jnp.mean(centered * centered, axis=-1, keepdims=True)
    return (centered * lax.rsqrt(variance + 1e-5) * gain_vec + shift_vec).astype(BF16)


def attn_kernel(heads, head_dim, qkv_ref, qm_ref, km_ref, out_ref):
    seq = qkv_ref.shape[0]
    width = heads * head_dim
    scale = head_dim ** -0.5 * LOG2E
    row = lax.broadcasted_iota(jnp.int32, (QB, QB), 0)
    col = lax.broadcasted_iota(jnp.int32, (QB, QB), 1)
    diag = jnp.where(col <= row, 0.0, -8e30).astype(F32)
    for i in reversed(range(seq // QB)):
        outs = []
        lo, hi = i * QB, (i + 1) * QB
        for h in range(heads):
            a, b = h * head_dim, (h + 1) * head_dim
            q = jnp.concatenate([qkv_ref[lo:hi, a:b], qm_ref[lo:hi, :]], axis=1)
            k = jnp.concatenate([qkv_ref[0:hi, width + a:width + b], km_ref[0:hi, :]], axis=1)
            s = lax.dot_general(q, k, (((1,), (1,)), ((), ())), preferred_element_type=F32)
            sd = s[:, lo:] + diag
            s = jnp.concatenate([s[:, :lo], sd], axis=1) if i else sd
            m = jnp.max(s, axis=1, keepdims=True)
            e = jnp.exp2((s - m) * scale)
            total = jnp.sum(e, axis=1, keepdims=True)
            p = (e * (1.0 / total)).astype(BF16)
            outs.append(jnp.dot(p, qkv_ref[0:hi, 2 * width + a:2 * width + b], preferred_element_type=F32))
        out_ref[lo:hi, :] = jnp.concatenate(outs, axis=1).astype(BF16)


def attention(qkv, q_mask, k_mask, heads, head_dim):
    seq = qkv.shape[0]

    def body(*refs):
        attn_kernel(heads, head_dim, *refs)

    vm = pl.BlockSpec(memory_space=pltpu.VMEM)
    return pl.pallas_call(
        body,
        out_shape=jax.ShapeDtypeStruct((seq, heads * head_dim), BF16),
        in_specs=[vm] * 3,
        out_specs=vm,
        name="doc_attention",
        cost_estimate=pl.CostEstimate(flops=20_000_000_000, bytes_accessed=5_000_000, transcendentals=0),
        compiler_params=pltpu.CompilerParams(vmem_limit_bytes=48 * 1024 * 1024),
    )(qkv, q_mask, k_mask)


def scatter_sum(partial_rows, groups):
    seq_len, model_dim = partial_rows.shape
    split_rows = partial_rows.reshape(groups, seq_len // groups, model_dim)
    received = lax.all_to_all(split_rows, "tp", 0, 0, tiled=True)
    return jnp.sum(received, axis=0, dtype=F32)


def solution(mesh):
    groups = mesh.shape["tp"]
    row_spec = P("dp", "tp", None)
    vec_spec = P(None, None)
    in_specs = (row_spec, P("dp", "tp"), vec_spec, vec_spec, P(None, None, None, "tp", None), P(None, "tp", None, None), vec_spec, vec_spec, vec_spec, P(None, None, "tp"), P(None, "tp"), P(None, "tp", None), vec_spec)

    def device_fn(tokens, doc_ids, norm1_gain, norm1_shift, qkv_weight, out_weight, out_bias, norm2_gain, norm2_shift, up_weight, up_bias, down_weight, down_bias):
        layers, model_dim, _, heads, head_dim = qkv_weight.shape
        width = heads * head_dim
        rows = tokens.shape[1]
        all_ids = lax.all_gather(doc_ids[0], "tp", axis=0, tiled=True)
        same = all_ids[:, None] == jnp.arange(head_dim, dtype=jnp.int32)[None, :]
        q_mask = jnp.where(same, -8e30, 0.0).astype(BF16)
        k_mask = jnp.where(same, 0.0, 1.0).astype(BF16)
        w_out = lax.all_gather(out_weight.reshape(layers, width, model_dim), "tp", axis=0, tiled=False)
        residual = tokens[0].astype(F32)
        for layer_idx in range(layers):
            normed = layer_norm(residual, norm1_gain[layer_idx], norm1_shift[layer_idx])
            full_rows = lax.all_gather(normed, "tp", axis=0, tiled=True)
            w_qkv = qkv_weight[layer_idx].reshape(model_dim, 3 * width)
            qkv = jnp.dot(full_rows, w_qkv, preferred_element_type=F32).astype(BF16)
            attn_out = attention(qkv, q_mask, k_mask, heads, head_dim)
            mine = lax.all_to_all(attn_out.reshape(groups, rows, width), "tp", 0, 0, tiled=True)
            parts = jnp.einsum("gsk,gkd->gsd", mine, w_out[:, layer_idx], preferred_element_type=F32).astype(BF16)
            residual = residual + (jnp.sum(parts, axis=0, dtype=F32) + out_bias[layer_idx])
            normed2 = layer_norm(residual, norm2_gain[layer_idx], norm2_shift[layer_idx])
            full_rows2 = lax.all_gather(normed2, "tp", axis=0, tiled=True)
            pre_act = jnp.dot(full_rows2, up_weight[layer_idx], preferred_element_type=F32) + up_bias[layer_idx]
            hidden = jax.nn.gelu(pre_act, approximate=True).astype(BF16)
            mlp_part = jnp.dot(hidden, down_weight[layer_idx], preferred_element_type=F32).astype(BF16)
            residual = residual + (scatter_sum(mlp_part, groups) + down_bias[layer_idx])
        return residual.astype(BF16)[None]

    return jax.shard_map(device_fn, mesh=mesh, in_specs=in_specs, out_specs=row_spec, check_vma=False)
```

```python
import jax
import jax.numpy as jnp
from jax import lax
from jax.experimental import pallas as pl
from jax.experimental.pallas import tpu as pltpu
from jax.sharding import PartitionSpec as P

F32 = jnp.float32
BF16 = jnp.bfloat16
QB = 256
LOG2E = 1.4426950408889634


def layer_norm(residual, gain_vec, shift_vec):
    mean_val = jnp.mean(residual, axis=-1, keepdims=True)
    centered = residual - mean_val
    variance = jnp.mean(centered * centered, axis=-1, keepdims=True)
    return (centered * lax.rsqrt(variance + 1e-5) * gain_vec + shift_vec).astype(BF16)


def attn_kernel(heads, head_dim, qkv_ref, qm_ref, km_ref, out_ref):
    seq = qkv_ref.shape[0]
    width = heads * head_dim
    scale = head_dim ** -0.5 * LOG2E
    row = lax.broadcasted_iota(jnp.int32, (QB, QB), 0)
    col = lax.broadcasted_iota(jnp.int32, (QB, QB), 1)
    diag = jnp.where(col <= row, 0.0, -8e30).astype(F32)
    for i in reversed(range(seq // QB)):
        outs = []
        lo, hi = i * QB, (i + 1) * QB
        for h in range(heads):
            a, b = h * head_dim, (h + 1) * head_dim
            q = jnp.concatenate([qkv_ref[lo:hi, a:b], qm_ref[lo:hi, :]], axis=1)
            k = jnp.concatenate([qkv_ref[0:hi, width + a:width + b], km_ref[0:hi, :]], axis=1)
            s = lax.dot_general(q, k, (((1,), (1,)), ((), ())), preferred_element_type=F32)
            sd = s[:, lo:] + diag
            s = jnp.concatenate([s[:, :lo], sd], axis=1) if i else sd
            m = jnp.max(s, axis=1, keepdims=True)
            e = jnp.exp2((s - m) * scale)
            total = jnp.sum(e, axis=1, keepdims=True)
            p = (e * (1.0 / total)).astype(BF16)
            outs.append(jnp.dot(p, qkv_ref[0:hi, 2 * width + a:2 * width + b], preferred_element_type=F32))
        out_ref[lo:hi, :] = jnp.concatenate(outs, axis=1).astype(BF16)


def attention(qkv, q_mask, k_mask, heads, head_dim):
    seq = qkv.shape[0]

    def body(*refs):
        attn_kernel(heads, head_dim, *refs)

    vm = pl.BlockSpec(memory_space=pltpu.VMEM)
    return pl.pallas_call(
        body,
        out_shape=jax.ShapeDtypeStruct((seq, heads * head_dim), BF16),
        in_specs=[vm] * 3,
        out_specs=vm,
        name="doc_attention",
        cost_estimate=pl.CostEstimate(flops=20_000_000_000, bytes_accessed=5_000_000, transcendentals=0),
        compiler_params=pltpu.CompilerParams(vmem_limit_bytes=48 * 1024 * 1024),
    )(qkv, q_mask, k_mask)


HALF = 128
CH = 64
OWN, LEFT, RIGHT, OPP = 0, 1, 2, 3
MESH_ID = pl.DeviceIdType.MESH


class Peers:
    def __init__(self, n):
        me = lax.axis_index("tp")
        chips = n // 2
        self.k = lax.rem(me, 2)
        chip = me // 2
        self.right = lax.rem(chip + 1, chips)
        self.left = lax.rem(chip + chips - 1, chips)
        self.chip = chip
        self.chips = chips
        self.opp = lax.rem(chip + 2, chips)

    def dev(self, chip, core):
        return {"tp": 2 * chip + core}

    @property
    def sib(self):
        return {"tp": 2 * self.chip + 1 - self.k}

    def greet(self):
        barrier = pltpu.get_barrier_semaphore()
        for d in (self.sib, self.dev(self.left, 0), self.dev(self.left, 1), self.dev(self.right, 0), self.dev(self.right, 1)):
            pl.semaphore_signal(barrier, inc=1, device_id=d, device_id_type=MESH_ID)

    def met(self):
        pl.semaphore_wait(pltpu.get_barrier_semaphore(), 5)


class Copies:
    def __init__(self):
        self.sent = []

    def send(self, src, dst, ss, rs, device):
        c = pltpu.make_async_remote_copy(src_ref=src, dst_ref=dst, send_sem=ss, recv_sem=rs, device_id=device, device_id_type=MESH_ID)
        c.start()
        self.sent.append(c)

    def recv(self, dst, ss, rs, device):
        pltpu.make_async_remote_copy(src_ref=dst, dst_ref=dst, send_sem=ss, recv_sem=rs, device_id=device, device_id_type=MESH_ID).wait_recv()

    def drain(self):
        for c in self.sent:
            c.wait_send()


class Gather:
    def __init__(self, peers, copies, buf, ss, rs):
        self.p, self.c, self.buf, self.ss, self.rs = peers, copies, buf, ss, rs

    def at(self, place, c, core):
        return self.buf.at[2 * place + c // 2, core, pl.ds((c % 2) * CH, CH), :]

    def start(self, c):
        p, k = self.p, self.p.k
        src = self.at(OWN, c, k)
        self.c.send(src, self.at(LEFT, c, k), self.ss.at[0, c], self.rs.at[0, c], p.dev(p.right, k))
        self.c.send(src, self.at(RIGHT, c, k), self.ss.at[1, c], self.rs.at[1, c], p.dev(p.left, k))
        self.c.send(src, src, self.ss.at[2, c], self.rs.at[2, c], p.sib)

    def wait(self, kind, place, c, core):
        self.c.recv(self.at(place, c, core), self.ss.at[kind, c], self.rs.at[kind, c], self.p.sib)

    def wait_sibling(self, c):
        self.wait(2, OWN, c, 1 - self.p.k)

    def near(self, c):
        p, k = self.p, self.p.k
        self.wait(0, LEFT, c, k)
        self.wait(1, RIGHT, c, k)
        self.c.send(self.at(1 + k, c, k), self.at(OPP, c, k), self.ss.at[5, c], self.rs.at[5, c], p.dev(lax.rem(p.chip + p.chips + 1 - 2 * k, p.chips), k))
        self.c.send(self.at(LEFT, c, k), self.at(LEFT, c, k), self.ss.at[3, c], self.rs.at[3, c], p.sib)
        self.c.send(self.at(RIGHT, c, k), self.at(RIGHT, c, k), self.ss.at[4, c], self.rs.at[4, c], p.sib)

    def near_sibling(self, c):
        self.wait(3, LEFT, c, 1 - self.p.k)
        self.wait(4, RIGHT, c, 1 - self.p.k)

    def far(self, c):
        k = self.p.k
        self.wait(5, OPP, c, k)
        self.c.send(self.at(OPP, c, k), self.at(OPP, c, k), self.ss.at[6, c], self.rs.at[6, c], self.p.sib)

    def far_sibling(self, c):
        self.wait(6, OPP, c, 1 - self.p.k)


def norm_rows(res_ref, gain, shift, buf, k):
    for c in range(4):
        x = res_ref[c * CH:(c + 1) * CH, :]
        mean = jnp.mean(x, axis=1, keepdims=True)
        cen = x - mean
        var = jnp.mean(cen * cen, axis=1, keepdims=True)
        h = (cen * lax.rsqrt(var + 1e-5) * gain + shift).astype(BF16)
        buf[c // 2, k, pl.ds((c % 2) * CH, CH), :] = h


def mlp_kernel(n, layer, res_ref, gain_ref, shift_ref, up_hbm, ub_ref, down_hbm, db_ref, out_ref,
               buf, part, hid, w_up, w_down, sibp, direct, midr, omid, msum, fin,
               w_sem, ag_ss, ag_rs, d_ss, d_rs, s_ss, s_rs, m_ss, m_rs, o_ss, o_rs, f_ss, f_rs):
    p = Peers(n)
    k = p.k
    p.greet()
    load_up = pltpu.make_async_copy(up_hbm.at[layer], w_up, w_sem.at[0])
    load_down = pltpu.make_async_copy(down_hbm.at[layer], w_down, w_sem.at[1])
    load_up.start()
    load_down.start()
    norm_rows(res_ref, gain_ref[layer:layer + 1, :], shift_ref[layer:layer + 1, :], buf, k)
    copies = Copies()
    g = Gather(p, copies, buf, ag_ss, ag_rs)
    p.met()
    for c in range(4):
        g.start(c)
    load_up.wait()
    load_down.wait()
    ff = w_up.shape[1]
    dm = w_down.shape[1]
    UN, DN = 512, 512
    rows = 2 * HALF

    def unit(u):
        def up(j, _):
            cols = pl.ds(pl.multiple_of(j * UN, UN), UN)
            x = buf[u].reshape(rows, dm)
            a = jnp.dot(x, w_up[:, cols], preferred_element_type=F32) + ub_ref[layer:layer + 1, cols]
            cdf = 0.5 * (1.0 + jnp.tanh(0.7978845608028654 * (a + 0.044715 * (a * a * a))))
            hid[:, cols] = (a * cdf).astype(BF16)
            return 0

        def down(j, _):
            cols = pl.ds(pl.multiple_of(j * DN, DN), DN)
            y = jnp.dot(hid[...], w_down[:, cols], preferred_element_type=F32).astype(BF16)
            part[u, :, :, cols] = y.reshape(2, HALF, DN)
            return 0

        lax.fori_loop(0, ff // UN, up, 0)
        lax.fori_loop(0, dm // DN, down, 0)

    def pair(s):
        def one(i, _):
            unit(2 + s + 2 * i)
            return 0
        lax.fori_loop(0, 2, one, 0)

    def send_direct(s):
        copies.send(part.at[2 * RIGHT + s, 1], direct.at[k, s], d_ss.at[0, s], d_rs.at[k, s], p.dev(p.right, 1))
        copies.send(part.at[2 * LEFT + s, 0], direct.at[k, s], d_ss.at[1, s], d_rs.at[k, s], p.dev(p.left, 0))

    for c in range(4):
        g.wait_sibling(c)
    unit(0)
    g.near(0)
    unit(1)
    g.near(1)
    for s in range(2):
        copies.send(part.at[s, 1 - k], sibp.at[s], s_ss.at[s], s_rs.at[s], p.sib)
    g.near_sibling(0)
    g.near_sibling(1)
    pair(0)
    g.near(2)
    g.near(3)
    send_direct(0)
    g.near_sibling(2)
    g.near_sibling(3)
    pair(1)
    send_direct(1)
    copies.send(part.at[2 * RIGHT + 1 - k, 0], midr.at[0], m_ss.at[0], m_rs.at[0], p.sib)
    copies.send(part.at[2 * LEFT + 1 - k, 1], midr.at[1], m_ss.at[1], m_rs.at[1], p.sib)
    for s in range(2):
        g.far(2 * s)
        g.far(2 * s + 1)
        g.far_sibling(2 * s)
        g.far_sibling(2 * s + 1)
        unit(2 * OPP + s)
        for j in range(2):
            r = pl.ds(j * CH, CH)
            copies.send(part.at[2 * OPP + s, 0, r, :], omid.at[0, k, r, :], o_ss.at[0, s, j], o_rs.at[0, k, j], p.dev(p.right, s))
            copies.send(part.at[2 * OPP + s, 1, r, :], omid.at[1, k, r, :], o_ss.at[1, s, j], o_rs.at[1, k, j], p.dev(p.left, s))
    for e in range(2):
        copies.recv(midr.at[e], m_ss.at[e], m_rs.at[e], p.sib)
    for j in range(2):
        r = pl.ds(j * CH, CH)
        for e in range(2):
            for q in range(2):
                copies.recv(omid.at[e, q, r, :], o_ss.at[e, q, j], o_rs.at[e, q, j], p.sib)
            own = part[2 * (RIGHT if e == 0 else LEFT) + k, e, r, :].astype(F32)
            msum[e, r, :] = (own + midr[e, r, :].astype(F32)) + (omid[e, 0, r, :].astype(F32) + omid[e, 1, r, :].astype(F32))
            copies.send(msum.at[e, r, :], fin.at[k, r, :], f_ss.at[e, j], f_rs.at[k, j], p.dev(p.right, 0) if e == 0 else p.dev(p.left, 1))
    for s in range(2):
        copies.recv(sibp.at[s], s_ss.at[s], s_rs.at[s], p.sib)
        for q in range(2):
            copies.recv(direct.at[q, s], d_ss.at[q, s], d_rs.at[q, s], p.sib)
    for j in range(2):
        r = pl.ds(j * CH, CH)
        for s in range(2):
            copies.recv(fin.at[s, r, :], f_ss.at[s, j], f_rs.at[s, j], p.sib)
            total = (part[s, k, r, :].astype(F32) + sibp[s, r, :].astype(F32)) + (direct[0, s, r, :].astype(F32) + direct[1, s, r, :].astype(F32)) + fin[s, r, :]
            o = pl.ds(s * HALF + j * CH, CH)
            out_ref[o, :] = res_ref[o, :] + (total + db_ref[layer:layer + 1, :])
    copies.drain()


def mlp(n, layer, residual, gain, shift, up_w, up_b, down_w, down_b):
    rows, dm = residual.shape
    ff = up_w.shape[2]

    def body(*refs):
        mlp_kernel(n, layer, *refs)

    vm = pl.BlockSpec(memory_space=pltpu.VMEM)
    hb = pl.BlockSpec(memory_space=pl.ANY)
    dma = pltpu.SemaphoreType.DMA
    return pl.pallas_call(
        body,
        out_shape=jax.ShapeDtypeStruct((rows, dm), F32),
        in_specs=[vm, vm, vm, hb, vm, hb, vm],
        out_specs=vm,
        scratch_shapes=[
            pltpu.VMEM((8, 2, HALF, dm), BF16),
            pltpu.VMEM((8, 2, HALF, dm), BF16),
            pltpu.VMEM((2 * HALF, ff), BF16),
            pltpu.VMEM((dm, ff), BF16),
            pltpu.VMEM((ff, dm), BF16),
            pltpu.VMEM((2, HALF, dm), BF16),
            pltpu.VMEM((2, 2, HALF, dm), BF16),
            pltpu.VMEM((2, HALF, dm), BF16),
            pltpu.VMEM((2, 2, HALF, dm), BF16),
            pltpu.VMEM((2, HALF, dm), F32),
            pltpu.VMEM((2, HALF, dm), F32),
            dma((2,)), dma((7, 4)), dma((7, 4)), dma((2, 2)), dma((2, 2)), dma((2,)), dma((2,)), dma((2,)), dma((2,)),
            dma((2, 2, 2)), dma((2, 2, 2)), dma((2, 2)), dma((2, 2)),
        ],
        name=f"mlp_{layer}",
        cost_estimate=pl.CostEstimate(flops=80_000_000_000, bytes_accessed=20_000_000, transcendentals=0),
        compiler_params=pltpu.CompilerParams(collective_id=10 + layer, has_side_effects=True, vmem_limit_bytes=60 * 1024 * 1024),
    )(residual, gain, shift, up_w, up_b, down_w, down_b)


def solution(mesh):
    groups = mesh.shape["tp"]
    row_spec = P("dp", "tp", None)
    vec_spec = P(None, None)
    in_specs = (row_spec, P("dp", "tp"), vec_spec, vec_spec, P(None, None, None, "tp", None), P(None, "tp", None, None), vec_spec, vec_spec, vec_spec, P(None, None, "tp"), P(None, "tp"), P(None, "tp", None), vec_spec)

    def device_fn(tokens, doc_ids, norm1_gain, norm1_shift, qkv_weight, out_weight, out_bias, norm2_gain, norm2_shift, up_weight, up_bias, down_weight, down_bias):
        layers, model_dim, _, heads, head_dim = qkv_weight.shape
        width = heads * head_dim
        rows = tokens.shape[1]
        all_ids = lax.all_gather(doc_ids[0], "tp", axis=0, tiled=True)
        same = all_ids[:, None] == jnp.arange(head_dim, dtype=jnp.int32)[None, :]
        q_mask = jnp.where(same, -8e30, 0.0).astype(BF16)
        k_mask = jnp.where(same, 0.0, 1.0).astype(BF16)
        w_out = lax.all_gather(out_weight.reshape(layers, width, model_dim), "tp", axis=0, tiled=False)
        residual = tokens[0].astype(F32)
        for layer_idx in range(layers):
            normed = layer_norm(residual, norm1_gain[layer_idx], norm1_shift[layer_idx])
            full_rows = lax.all_gather(normed, "tp", axis=0, tiled=True)
            w_qkv = qkv_weight[layer_idx].reshape(model_dim, 3 * width)
            qkv = jnp.dot(full_rows, w_qkv, preferred_element_type=F32).astype(BF16)
            attn_out = attention(qkv, q_mask, k_mask, heads, head_dim)
            mine = lax.all_to_all(attn_out.reshape(groups, rows, width), "tp", 0, 0, tiled=True)
            parts = jnp.einsum("gsk,gkd->gsd", mine, w_out[:, layer_idx], preferred_element_type=F32).astype(BF16)
            residual = residual + (jnp.sum(parts, axis=0, dtype=F32) + out_bias[layer_idx])
            residual = mlp(groups, layer_idx, residual, norm2_gain, norm2_shift, up_weight, up_bias, down_weight, down_bias)
        return residual.astype(BF16)[None]

    return jax.shard_map(device_fn, mesh=mesh, in_specs=in_specs, out_specs=row_spec, check_vma=False)
```

```python
import jax
import jax.numpy as jnp
from jax import lax
from jax.experimental import pallas as pl
from jax.experimental.pallas import tpu as pltpu
from jax.sharding import PartitionSpec as P

F32 = jnp.float32
BF16 = jnp.bfloat16
HALF = 128
CH = 64
OWN, LEFT, RIGHT, OPP = 0, 1, 2, 3
MESH_ID = pl.DeviceIdType.MESH


class Peers:
    def __init__(self, n):
        me = lax.axis_index("tp")
        chips = n // 2
        self.k = lax.rem(me, 2)
        chip = me // 2
        self.right = lax.rem(chip + 1, chips)
        self.left = lax.rem(chip + chips - 1, chips)
        self.chip = chip
        self.chips = chips
        self.opp = lax.rem(chip + 2, chips)

    def dev(self, chip, core):
        return {"tp": 2 * chip + core}

    @property
    def sib(self):
        return {"tp": 2 * self.chip + 1 - self.k}

    def greet(self):
        barrier = pltpu.get_barrier_semaphore()
        for d in (self.sib, self.dev(self.left, 0), self.dev(self.left, 1), self.dev(self.right, 0), self.dev(self.right, 1)):
            pl.semaphore_signal(barrier, inc=1, device_id=d, device_id_type=MESH_ID)

    def greet_all(self, n):
        barrier = pltpu.get_barrier_semaphore()
        for d in range(1, n):
            other = lax.rem(2 * self.chip + self.k + d, n)
            pl.semaphore_signal(barrier, inc=1, device_id={"tp": other}, device_id_type=MESH_ID)

    def met_all(self, n):
        pl.semaphore_wait(pltpu.get_barrier_semaphore(), n - 1)

    def met(self):
        pl.semaphore_wait(pltpu.get_barrier_semaphore(), 5)


class Copies:
    def __init__(self):
        self.sent = []

    def send(self, src, dst, ss, rs, device):
        c = pltpu.make_async_remote_copy(src_ref=src, dst_ref=dst, send_sem=ss, recv_sem=rs, device_id=device, device_id_type=MESH_ID)
        c.start()
        self.sent.append(c)

    def recv(self, dst, ss, rs, device):
        pltpu.make_async_remote_copy(src_ref=dst, dst_ref=dst, send_sem=ss, recv_sem=rs, device_id=device, device_id_type=MESH_ID).wait_recv()

    def drain(self):
        for c in self.sent:
            c.wait_send()


class Gather:
    def __init__(self, peers, copies, buf, ss, rs):
        self.p, self.c, self.buf, self.ss, self.rs = peers, copies, buf, ss, rs

    def at(self, place, c, core):
        return self.buf.at[2 * place + c // 2, core, pl.ds((c % 2) * CH, CH), :]

    def start(self, c):
        p, k = self.p, self.p.k
        src = self.at(OWN, c, k)
        self.c.send(src, self.at(LEFT, c, k), self.ss.at[0, c], self.rs.at[0, c], p.dev(p.right, k))
        self.c.send(src, self.at(RIGHT, c, k), self.ss.at[1, c], self.rs.at[1, c], p.dev(p.left, k))
        self.c.send(src, src, self.ss.at[2, c], self.rs.at[2, c], p.sib)

    def wait(self, kind, place, c, core):
        self.c.recv(self.at(place, c, core), self.ss.at[kind, c], self.rs.at[kind, c], self.p.sib)

    def wait_sibling(self, c):
        self.wait(2, OWN, c, 1 - self.p.k)

    def near(self, c):
        p, k = self.p, self.p.k
        self.wait(0, LEFT, c, k)
        self.wait(1, RIGHT, c, k)
        self.c.send(self.at(1 + k, c, k), self.at(OPP, c, k), self.ss.at[5, c], self.rs.at[5, c], p.dev(lax.rem(p.chip + p.chips + 1 - 2 * k, p.chips), k))
        self.c.send(self.at(LEFT, c, k), self.at(LEFT, c, k), self.ss.at[3, c], self.rs.at[3, c], p.sib)
        self.c.send(self.at(RIGHT, c, k), self.at(RIGHT, c, k), self.ss.at[4, c], self.rs.at[4, c], p.sib)

    def near_sibling(self, c):
        self.wait(3, LEFT, c, 1 - self.p.k)
        self.wait(4, RIGHT, c, 1 - self.p.k)

    def far(self, c):
        k = self.p.k
        self.wait(5, OPP, c, k)
        self.c.send(self.at(OPP, c, k), self.at(OPP, c, k), self.ss.at[6, c], self.rs.at[6, c], self.p.sib)

    def far_sibling(self, c):
        self.wait(6, OPP, c, 1 - self.p.k)


def norm_rows(res_ref, gain, shift, buf, k):
    for c in range(4):
        x = res_ref[c * CH:(c + 1) * CH, :].astype(F32)
        mean = jnp.mean(x, axis=1, keepdims=True)
        cen = x - mean
        var = jnp.mean(cen * cen, axis=1, keepdims=True)
        h = (cen * lax.rsqrt(var + 1e-5) * gain + shift).astype(BF16)
        buf[c // 2, k, pl.ds((c % 2) * CH, CH), :] = h


def mlp_kernel(n, layer, res_ref, gain_ref, shift_ref, up_hbm, ub_ref, down_hbm, db_ref, out_ref,
               buf, part, hid, w_up, w_down, sibp, direct, midr, omid, msum, fin,
               w_sem, ag_ss, ag_rs, d_ss, d_rs, s_ss, s_rs, m_ss, m_rs, o_ss, o_rs, f_ss, f_rs):
    p = Peers(n)
    k = p.k
    p.greet()
    load_up = pltpu.make_async_copy(up_hbm.at[layer], w_up, w_sem.at[0])
    load_down = pltpu.make_async_copy(down_hbm.at[layer], w_down, w_sem.at[1])
    load_up.start()
    load_down.start()
    norm_rows(res_ref, gain_ref[layer:layer + 1, :], shift_ref[layer:layer + 1, :], buf, k)
    copies = Copies()
    g = Gather(p, copies, buf, ag_ss, ag_rs)
    p.met()
    for c in range(4):
        g.start(c)
    load_up.wait()
    load_down.wait()
    ff = w_up.shape[1]
    dm = w_down.shape[1]
    UN, DN = 512, 512
    rows = 2 * HALF

    def unit(u):
        def up(j, _):
            cols = pl.ds(pl.multiple_of(j * UN, UN), UN)
            x = buf[u].reshape(rows, dm)
            a = jnp.dot(x, w_up[:, cols], preferred_element_type=F32) + ub_ref[layer:layer + 1, cols]
            cdf = 0.5 * (1.0 + jnp.tanh(0.7978845608028654 * (a + 0.044715 * (a * a * a))))
            hid[:, cols] = (a * cdf).astype(BF16)
            return 0

        def down(j, _):
            cols = pl.ds(pl.multiple_of(j * DN, DN), DN)
            y = jnp.dot(hid[...], w_down[:, cols], preferred_element_type=F32).astype(BF16)
            part[u, :, :, cols] = y.reshape(2, HALF, DN)
            return 0

        lax.fori_loop(0, ff // UN, up, 0)
        lax.fori_loop(0, dm // DN, down, 0)

    def pair(s):
        def one(i, _):
            unit(2 + s + 2 * i)
            return 0
        lax.fori_loop(0, 2, one, 0)

    def send_direct(s):
        copies.send(part.at[2 * RIGHT + s, 1], direct.at[k, s], d_ss.at[0, s], d_rs.at[k, s], p.dev(p.right, 1))
        copies.send(part.at[2 * LEFT + s, 0], direct.at[k, s], d_ss.at[1, s], d_rs.at[k, s], p.dev(p.left, 0))

    for c in range(4):
        g.wait_sibling(c)
    unit(0)
    g.near(0)
    unit(1)
    g.near(1)
    for s in range(2):
        copies.send(part.at[s, 1 - k], sibp.at[s], s_ss.at[s], s_rs.at[s], p.sib)
    g.near_sibling(0)
    g.near_sibling(1)
    pair(0)
    g.near(2)
    g.near(3)
    send_direct(0)
    g.near_sibling(2)
    g.near_sibling(3)
    pair(1)
    send_direct(1)
    copies.send(part.at[2 * RIGHT + 1 - k, 0], midr.at[0], m_ss.at[0], m_rs.at[0], p.sib)
    copies.send(part.at[2 * LEFT + 1 - k, 1], midr.at[1], m_ss.at[1], m_rs.at[1], p.sib)
    for s in range(2):
        g.far(2 * s)
        g.far(2 * s + 1)
        g.far_sibling(2 * s)
        g.far_sibling(2 * s + 1)
        unit(2 * OPP + s)
        for j in range(2):
            r = pl.ds(j * CH, CH)
            copies.send(part.at[2 * OPP + s, 0, r, :], omid.at[0, k, r, :], o_ss.at[0, s, j], o_rs.at[0, k, j], p.dev(p.right, s))
            copies.send(part.at[2 * OPP + s, 1, r, :], omid.at[1, k, r, :], o_ss.at[1, s, j], o_rs.at[1, k, j], p.dev(p.left, s))
    for e in range(2):
        copies.recv(midr.at[e], m_ss.at[e], m_rs.at[e], p.sib)
    for j in range(2):
        r = pl.ds(j * CH, CH)
        for e in range(2):
            for q in range(2):
                copies.recv(omid.at[e, q, r, :], o_ss.at[e, q, j], o_rs.at[e, q, j], p.sib)
            own = part[2 * (RIGHT if e == 0 else LEFT) + k, e, r, :].astype(F32)
            msum[e, r, :] = (own + midr[e, r, :].astype(F32)) + (omid[e, 0, r, :].astype(F32) + omid[e, 1, r, :].astype(F32))
            copies.send(msum.at[e, r, :], fin.at[k, r, :], f_ss.at[e, j], f_rs.at[k, j], p.dev(p.right, 0) if e == 0 else p.dev(p.left, 1))
    for s in range(2):
        copies.recv(sibp.at[s], s_ss.at[s], s_rs.at[s], p.sib)
        for q in range(2):
            copies.recv(direct.at[q, s], d_ss.at[q, s], d_rs.at[q, s], p.sib)
    for j in range(2):
        r = pl.ds(j * CH, CH)
        for s in range(2):
            copies.recv(fin.at[s, r, :], f_ss.at[s, j], f_rs.at[s, j], p.sib)
            total = (part[s, k, r, :].astype(F32) + sibp[s, r, :].astype(F32)) + (direct[0, s, r, :].astype(F32) + direct[1, s, r, :].astype(F32)) + fin[s, r, :]
            o = pl.ds(s * HALF + j * CH, CH)
            out_ref[o, :] = res_ref[o, :] + (total + db_ref[layer:layer + 1, :])
    copies.drain()


def mlp(n, layer, residual, gain, shift, up_w, up_b, down_w, down_b):
    rows, dm = residual.shape
    ff = up_w.shape[2]

    def body(*refs):
        mlp_kernel(n, layer, *refs)

    vm = pl.BlockSpec(memory_space=pltpu.VMEM)
    hb = pl.BlockSpec(memory_space=pl.ANY)
    dma = pltpu.SemaphoreType.DMA
    return pl.pallas_call(
        body,
        out_shape=jax.ShapeDtypeStruct((rows, dm), F32),
        in_specs=[vm, vm, vm, hb, vm, hb, vm],
        out_specs=vm,
        scratch_shapes=[
            pltpu.VMEM((8, 2, HALF, dm), BF16),
            pltpu.VMEM((8, 2, HALF, dm), BF16),
            pltpu.VMEM((2 * HALF, ff), BF16),
            pltpu.VMEM((dm, ff), BF16),
            pltpu.VMEM((ff, dm), BF16),
            pltpu.VMEM((2, HALF, dm), BF16),
            pltpu.VMEM((2, 2, HALF, dm), BF16),
            pltpu.VMEM((2, HALF, dm), BF16),
            pltpu.VMEM((2, 2, HALF, dm), BF16),
            pltpu.VMEM((2, HALF, dm), F32),
            pltpu.VMEM((2, HALF, dm), F32),
            dma((2,)), dma((7, 4)), dma((7, 4)), dma((2, 2)), dma((2, 2)), dma((2,)), dma((2,)), dma((2,)), dma((2,)),
            dma((2, 2, 2)), dma((2, 2, 2)), dma((2, 2)), dma((2, 2)),
        ],
        name=f"mlp_{layer}",
        cost_estimate=pl.CostEstimate(flops=80_000_000_000, bytes_accessed=20_000_000, transcendentals=0),
        compiler_params=pltpu.CompilerParams(collective_id=10 + layer, has_side_effects=True, vmem_limit_bytes=60 * 1024 * 1024),
    )(residual, gain, shift, up_w, up_b, down_w, down_b)


QB = 256
LOG2E = 1.4426950408889634
PAD = 128


def attn_kernel(n, layer, res_ref, gain_ref, shift_ref, hot_ref, qkv_hbm, wo_hbm, ob_ref, out_ref,
                buf, wbuf, w_qk, w_v, qk_s, v_s, qm_s, km_s, hots, heads_s, got,
                w_sem, h_ss, h_rs, ag_ss, ag_rs, wg_ss, wg_rs, a_ss, a_rs):
    p = Peers(n)
    k = p.k
    me = 2 * p.chip + k
    heads, dim = qkv_hbm.shape[2], qkv_hbm.shape[3]
    dm = res_ref.shape[1]
    width = heads * dim
    rows = 2 * HALF
    scale = dim ** -0.5 * LOG2E
    p.greet_all(n)
    loads = []
    for t in range(2):
        for h in range(heads):
            loads.append(pltpu.make_async_copy(qkv_hbm.at[layer, t, h], w_qk.at[t * heads + h, 0:dim, :], w_sem.at[t * heads + h]))
    for h in range(heads):
        loads.append(pltpu.make_async_copy(qkv_hbm.at[layer, 2, h], w_v.at[pl.ds(h * dim, dim), :], w_sem.at[2 * heads + h]))
    wloads = [pltpu.make_async_copy(wo_hbm.at[layer, pl.ds(s * HALF, HALF), :], wbuf.at[s, k], w_sem.at[3 * heads + s]) for s in range(2)]
    for c in loads + wloads:
        c.start()
    norm_rows(res_ref, gain_ref[layer:layer + 1, :], shift_ref[layer:layer + 1, :], buf, k)
    for t in range(2 * heads):
        w_qk[t, dim:PAD, :] = jnp.zeros((PAD - dim, dm), BF16)
    hots[me] = hot_ref[...]
    copies = Copies()
    g = Gather(p, copies, buf, ag_ss, ag_rs)
    gw = Gather(p, copies, wbuf, wg_ss, wg_rs)
    p.met_all(n)
    for d in range(1, n):
        copies.send(hot_ref, hots.at[me], h_ss.at[d - 1], h_rs.at[d - 1], {"tp": lax.rem(me + d, n)})
    for c in range(4):
        g.start(c)
    for c in loads + wloads:
        c.wait()
    for d in range(1, n):
        src = lax.rem(me + n - d, n)
        copies.recv(hots.at[src], h_ss.at[d - 1], h_rs.at[d - 1], p.sib)
    docs = hot_ref.shape[0]
    lane = lax.broadcasted_iota(jnp.int32, (docs, PAD), 1)
    place = lax.broadcasted_iota(jnp.int32, (docs, PAD), 0)
    pick = jnp.where(lane == place + dim, 1.0, 0.0).astype(BF16)
    lanes = lax.broadcasted_iota(jnp.int32, (QB, PAD), 1)
    used = jnp.where((lanes >= dim) & (lanes < dim + docs), 1.0, 0.0).astype(F32)
    for i in range(n):
        one = lax.dot_general(hots[i], pick, (((0,), (0,)), ((), ())), preferred_element_type=F32)
        qm_s[i * QB:(i + 1) * QB, :] = (one * -8e30).astype(BF16)
        km_s[i * QB:(i + 1) * QB, :] = (used - one).astype(BF16)

    def unit(u, chip):
        x = buf[u].reshape(rows, dm)
        half = u % 2 if isinstance(u, int) else lax.rem(u, 2)
        for t in range(2):
            w = w_qk[t * heads:(t + 1) * heads].reshape(heads * PAD, dm)
            y = lax.dot_general(x, w, (((1,), (1,)), ((), ())), preferred_element_type=F32)
            for kk in range(2):
                at = pl.ds(pl.multiple_of((2 * chip + kk) * rows + half * HALF, HALF), HALF)
                mask = (qm_s if t == 0 else km_s)[at, :].astype(F32)
                for h in range(heads):
                    part = y[kk * HALF:(kk + 1) * HALF, h * PAD:(h + 1) * PAD] + mask
                    qk_s[at, (t * heads + h) * PAD:(t * heads + h + 1) * PAD] = part.astype(BF16)
        y = lax.dot_general(x, w_v[...], (((1,), (1,)), ((), ())), preferred_element_type=F32).astype(BF16)
        for kk in range(2):
            at = pl.ds(pl.multiple_of((2 * chip + kk) * rows + half * HALF, HALF), HALF)
            v_s[at, :] = y[kk * HALF:(kk + 1) * HALF, :]

    def pair(s):
        def one(i, _):
            unit(2 + s + 2 * i, p.left + i * (p.right - p.left))
            return 0
        lax.fori_loop(0, 2, one, 0)

    for c in range(4):
        g.wait_sibling(c)
    unit(0, p.chip)
    g.near(0)
    unit(1, p.chip)
    g.near(1)
    g.near_sibling(0)
    g.near_sibling(1)
    pair(0)
    g.near(2)
    g.near(3)
    for c in range(4):
        gw.start(c)
    g.near_sibling(2)
    g.near_sibling(3)
    pair(1)
    for s in range(2):
        g.far(2 * s)
        g.far(2 * s + 1)
        g.far_sibling(2 * s)
        g.far_sibling(2 * s + 1)
        unit(2 * OPP + s, p.opp)

    row = lax.broadcasted_iota(jnp.int32, (QB, QB), 0)
    col = lax.broadcasted_iota(jnp.int32, (QB, QB), 1)
    diag = jnp.where(col <= row, 0.0, -8e30).astype(F32)
    low = lax.broadcasted_iota(jnp.int32, (1, PAD), 1) < dim

    def block(i):
        lo, hi = i * QB, (i + 1) * QB
        for gr in range(heads // 2):
            pair_v = v_s[0:hi, gr * PAD:(gr + 1) * PAD]
            zero = jnp.zeros_like(pair_v)
            out = None
            for b in range(2):
                h = 2 * gr + b
                q = qk_s[lo:hi, h * PAD:(h + 1) * PAD]
                kk = qk_s[0:hi, (heads + h) * PAD:(heads + h + 1) * PAD]
                s = lax.dot_general(q, kk, (((1,), (1,)), ((), ())), preferred_element_type=F32)
                sd = s[:, lo:] + diag
                s = jnp.concatenate([s[:, :lo], sd], axis=1) if i else sd
                m = jnp.max(s, axis=1, keepdims=True)
                e = jnp.exp2((s - m) * scale)
                total = jnp.sum(e, axis=1, keepdims=True)
                pr = (e * (1.0 / total)).astype(BF16)
                v = jnp.where(low, pair_v, zero) if b == 0 else jnp.where(low, zero, pair_v)
                o = jnp.dot(pr, v, preferred_element_type=F32)
                out = o if out is None else out + o
            heads_s[i, :, gr * PAD:(gr + 1) * PAD] = out.astype(BF16)

    def to_owner(i):
        return pltpu.make_async_remote_copy(src_ref=heads_s.at[i], dst_ref=got.at[me], send_sem=a_ss.at[i], recv_sem=a_rs.at[me], device_id={"tp": i}, device_id_type=MESH_ID)

    for i in range(n):
        block(i)

        @pl.when(me != i)
        def _():
            to_owner(i).start()

        if i == n // 2 - 1:
            gw.near(0)
        elif i == n - 3:
            gw.near(1)
        elif i == n - 2:
            gw.near(2)
    for c in range(4):
        gw.wait_sibling(c)
    gw.near(3)
    got[me] = heads_s[me]
    out_ref[...] = jnp.zeros_like(out_ref)
    DN = 512

    def project(o, chip, core):
        a = got[2 * chip + core]

        def tile(j, _):
            cols = pl.ds(pl.multiple_of(j * DN, DN), DN)
            w = wbuf[2 * o:2 * o + 2, core, :, cols].reshape(rows, DN)
            out_ref[:, cols] += jnp.dot(a, w, preferred_element_type=F32).astype(BF16).astype(F32)
            return 0

        lax.fori_loop(0, dm // DN, tile, 0)

    def arrive(src):
        pltpu.make_async_remote_copy(src_ref=got.at[src], dst_ref=got.at[src], send_sem=a_ss.at[src], recv_sem=a_rs.at[src], device_id=p.sib, device_id_type=MESH_ID).wait_recv()

    arrive(2 * p.chip + 1 - k)
    for kk in range(2):
        project(OWN, p.chip, kk)
    for c in range(4):
        gw.near_sibling(c)
    for o, chip in ((LEFT, p.left), (RIGHT, p.right)):
        for kk in range(2):
            arrive(2 * chip + kk)
            project(o, chip, kk)
    for c in range(4):
        gw.far(c)
    for c in range(4):
        gw.far_sibling(c)
    for kk in range(2):
        arrive(2 * p.opp + kk)
        project(OPP, p.opp, kk)
    out_ref[...] = res_ref[...].astype(F32) + (out_ref[...] + ob_ref[layer:layer + 1, :])
    copies.drain()
    for i in range(n):
        @pl.when(me != i)
        def _():
            to_owner(i).wait_send()


def attn_block(n, layer, residual, gain, shift, hot, qkv_w, out_w, out_b):
    rows, dm = residual.shape
    heads, dim = qkv_w.shape[2], qkv_w.shape[3]
    seq = n * rows

    def body(*refs):
        attn_kernel(n, layer, *refs)

    vm = pl.BlockSpec(memory_space=pltpu.VMEM)
    hb = pl.BlockSpec(memory_space=pl.ANY)
    dma = pltpu.SemaphoreType.DMA
    return pl.pallas_call(
        body,
        out_shape=jax.ShapeDtypeStruct((rows, dm), F32),
        in_specs=[vm, vm, vm, vm, hb, hb, vm],
        out_specs=vm,
        scratch_shapes=[
            pltpu.VMEM((8, 2, HALF, dm), BF16),
            pltpu.VMEM((8, 2, HALF, dm), BF16),
            pltpu.VMEM((2 * heads, PAD, dm), BF16),
            pltpu.VMEM((heads * dim, dm), BF16),
            pltpu.VMEM((seq, 2 * heads * PAD), BF16),
            pltpu.VMEM((seq, heads * dim), BF16),
            pltpu.VMEM((seq, PAD), BF16),
            pltpu.VMEM((seq, PAD), BF16),
            pltpu.VMEM((n,) + hot.shape, BF16),
            pltpu.VMEM((n, rows, heads * dim), BF16),
            pltpu.VMEM((n, rows, heads * dim), BF16),
            dma((3 * heads + 2,)), dma((n - 1,)), dma((n - 1,)), dma((7, 4)), dma((7, 4)), dma((7, 4)), dma((7, 4)), dma((n,)), dma((n,)),
        ],
        name=f"attn_{layer}",
        cost_estimate=pl.CostEstimate(flops=60_000_000_000, bytes_accessed=20_000_000, transcendentals=0),
        compiler_params=pltpu.CompilerParams(collective_id=20 + layer, has_side_effects=True, vmem_limit_bytes=62 * 1024 * 1024),
    )(residual, gain, shift, hot, qkv_w, out_w, out_b)


def solution(mesh):
    groups = mesh.shape["tp"]
    row_spec = P("dp", "tp", None)
    vec_spec = P(None, None)
    in_specs = (row_spec, P("dp", "tp"), vec_spec, vec_spec, P(None, None, None, "tp", None), P(None, "tp", None, None), vec_spec, vec_spec, vec_spec, P(None, None, "tp"), P(None, "tp"), P(None, "tp", None), vec_spec)

    def device_fn(tokens, doc_ids, norm1_gain, norm1_shift, qkv_weight, out_weight, out_bias, norm2_gain, norm2_shift, up_weight, up_bias, down_weight, down_bias):
        layers, model_dim, _, heads, head_dim = qkv_weight.shape
        hot = (jnp.arange(16, dtype=jnp.int32)[:, None] == doc_ids).astype(BF16)
        qkv_t = jnp.transpose(qkv_weight, (0, 2, 3, 4, 1))
        out_w = out_weight.reshape(layers, heads * head_dim, model_dim)
        residual = tokens[0]
        for layer in range(layers):
            residual = attn_block(groups, layer, residual, norm1_gain, norm1_shift, hot, qkv_t, out_w, out_bias)
            residual = mlp(groups, layer, residual, norm2_gain, norm2_shift, up_weight, up_bias, down_weight, down_bias)
        return residual.astype(BF16)[None]

    return jax.shard_map(device_fn, mesh=mesh, in_specs=in_specs, out_specs=row_spec, check_vma=False)
```

```python
import jax
import jax.numpy as jnp
from jax import lax
from jax.experimental import pallas as pl
from jax.experimental.pallas import tpu as pltpu
from jax.sharding import PartitionSpec as P

F32 = jnp.float32
BF16 = jnp.bfloat16
HALF = 128
CH = 64
WCH = 32
QB = 256
PAD = 128
LOG2E = 1.4426950408889634
OWN, LEFT, RIGHT, OPP = 0, 1, 2, 3
MESH_ID = pl.DeviceIdType.MESH


def slot(place, s):
    return {OWN: s, LEFT: 2 + 2 * s, RIGHT: 3 + 2 * s, OPP: 6 + s}[place]


class Peers:
    def __init__(self, n):
        self.n = n
        self.me = lax.axis_index("tp")
        chips = n // 2
        self.k = lax.rem(self.me, 2)
        self.chip = self.me // 2
        self.right = lax.rem(self.chip + 1, chips)
        self.left = lax.rem(self.chip + chips - 1, chips)
        self.opp = lax.rem(self.chip + 2, chips)
        self.onward = lax.rem(self.chip + chips + 1 - 2 * self.k, chips)
        dp = lax.axis_index("dp")
        self.side = lax.rem(dp, 2)
        self.twin = {"dp": dp + 1 - 2 * self.side, "tp": self.me}
        self.sib = {"tp": 2 * self.chip + 1 - self.k}
        self.to_right = [{"tp": 2 * self.right + c} for c in (0, 1)]
        self.to_left = [{"tp": 2 * self.left + c} for c in (0, 1)]
        self.same_right = {"tp": 2 * self.right + self.k}
        self.same_left = {"tp": 2 * self.left + self.k}
        self.same_onward = {"tp": 2 * self.onward + self.k}


    def greet(self, sem):
        for d in range(1, self.n):
            pl.semaphore_signal(sem, inc=1, device_id={"tp": lax.rem(self.me + d, self.n)}, device_id_type=MESH_ID)
        pl.semaphore_signal(sem, inc=1, device_id=self.twin, device_id_type=MESH_ID)

    def met(self, sem):
        pl.semaphore_wait(sem, self.n)


def copy(src, dst, ss, rs, device):
    return pltpu.make_async_remote_copy(src_ref=src, dst_ref=dst, send_sem=ss, recv_sem=rs, device_id=device, device_id_type=MESH_ID)


class Copies:
    def __init__(self, p):
        self.p = p
        self.sent = []

    def send(self, make):
        make().start()
        self.sent.append(make)

    def recv(self, dst, ss, rs):
        copy(dst, dst, ss, rs, self.p.sib).wait_recv()

    def drain(self):
        for make in self.sent:
            make().wait_send()
        self.sent = []


class Gather(Copies):
    def __init__(self, p, buf, ss, rs):
        super().__init__(p)
        self.buf, self.ss, self.rs = buf, ss, rs

    def at(self, place, c, core):
        return self.buf.at[slot(place, c // 2), core, pl.ds((c % 2) * CH, CH), :]

    def put(self, kind, c, src, dst, device):
        self.send(lambda: copy(src(), dst(), self.ss.at[kind, c], self.rs.at[kind, c], device))

    def take(self, kind, place, c, core):
        self.recv(self.at(place, c, core), self.ss.at[kind, c], self.rs.at[kind, c])

    def start(self, c):
        p, k = self.p, self.p.k
        own = lambda: self.at(OWN, c, k)
        self.put(0, c, own, lambda: self.at(LEFT, c, k), p.same_right)
        self.put(1, c, own, lambda: self.at(RIGHT, c, k), p.same_left)
        self.put(2, c, own, own, p.sib)

    def sibling(self, c):
        self.take(2, OWN, c, 1 - self.p.k)

    def near(self, c):
        p, k = self.p, self.p.k
        self.take(0, LEFT, c, k)
        self.take(1, RIGHT, c, k)
        ring = lambda: self.buf.at[2 + 2 * (c // 2) + k, k, pl.ds((c % 2) * CH, CH), :]
        self.put(5, c, ring, lambda: self.at(OPP, c, k), p.same_onward)
        self.put(3, c, lambda: self.at(LEFT, c, k), lambda: self.at(LEFT, c, k), p.sib)
        self.put(4, c, lambda: self.at(RIGHT, c, k), lambda: self.at(RIGHT, c, k), p.sib)

    def near_sibling(self, c):
        self.take(3, LEFT, c, 1 - self.p.k)
        self.take(4, RIGHT, c, 1 - self.p.k)

    def far(self, c):
        k = self.p.k
        self.take(5, OPP, c, k)
        self.put(6, c, lambda: self.at(OPP, c, k), lambda: self.at(OPP, c, k), self.p.sib)

    def far_sibling(self, c):
        self.take(6, OPP, c, 1 - self.p.k)


class WeightGather(Copies):
    def __init__(self, p, buf, ss, rs):
        super().__init__(p)
        self.buf, self.ss, self.rs = buf, ss, rs

    def mine(self, i):
        return i + 5 * self.p.side if i < 3 else i

    def theirs(self, i):
        return i + 5 * (1 - self.p.side)

    def at_slot(self, spot, c, core):
        start = (c % (HALF // WCH)) * WCH
        if not isinstance(start, int):
            start = pl.multiple_of(start, WCH)
        return self.buf.at[spot, core, pl.ds(start, WCH), :]

    def at(self, place, c, core):
        return self.at_slot(slot(place, c // (HALF // WCH)), c, core)

    def put(self, kind, c, src, dst, device):
        self.send(lambda: copy(src(c()), dst(c()), self.ss.at[kind, c()], self.rs.at[kind, c()], device))

    def take(self, kind, place, c, core):
        self.recv(self.at(place, c, core), self.ss.at[kind, c], self.rs.at[kind, c])

    def start(self):
        p, k = self.p, self.p.k
        for i in range(5):
            c = lambda i=i: self.mine(i)
            self.put(0, c, lambda c: self.at(OWN, c, k), lambda c: self.at(LEFT, c, k), p.same_right)
            self.put(1, c, lambda c: self.at(OWN, c, k), lambda c: self.at(RIGHT, c, k), p.same_left)
        for s in range(2):
            self.send(lambda s=s: copy(self.buf.at[s, k], self.buf.at[s, k], self.ss.at[2, s], self.rs.at[2, s], p.sib))

    def sibling(self):
        for s in range(2):
            self.recv(self.buf.at[s, 1 - self.p.k], self.ss.at[2, s], self.rs.at[2, s])

    def near(self, i):
        p, k = self.p, self.p.k
        c = lambda: self.mine(i)
        left = lambda c: self.at(LEFT, c, k)
        right = lambda c: self.at(RIGHT, c, k)
        self.take(0, LEFT, c(), k)
        self.take(1, RIGHT, c(), k)
        ring = lambda c: self.at_slot(2 + 2 * (c // (HALF // WCH)) + k, c, k)
        self.put(5, c, ring, lambda c: self.at(OPP, c, k), p.same_onward)
        if i < 3:
            self.put(7, c, left, left, p.twin)
            self.put(8, c, right, right, p.twin)
        self.put(3, c, left, left, p.sib)
        self.put(4, c, right, right, p.sib)

    def far(self, i):
        p, k = self.p, self.p.k
        c = lambda: self.mine(i)
        opp = lambda c: self.at(OPP, c, k)
        self.take(5, OPP, c(), k)
        if i < 3:
            self.put(9, c, opp, opp, p.twin)
        self.put(6, c, opp, opp, p.sib)

    def twin_near(self, i):
        p, k = self.p, self.p.k
        c = lambda: self.theirs(i)
        left = lambda c: self.at(LEFT, c, k)
        right = lambda c: self.at(RIGHT, c, k)
        self.take(7, LEFT, c(), k)
        self.take(8, RIGHT, c(), k)
        self.put(3, c, left, left, p.sib)
        self.put(4, c, right, right, p.sib)

    def twin_far(self, i):
        p, k = self.p, self.p.k
        c = lambda: self.theirs(i)
        opp = lambda c: self.at(OPP, c, k)
        self.take(9, OPP, c(), k)
        self.put(6, c, opp, opp, p.sib)

    def near_sibling(self):
        for c in range(8):
            self.take(3, LEFT, c, 1 - self.p.k)
            self.take(4, RIGHT, c, 1 - self.p.k)

    def far_sibling(self):
        for c in range(8):
            self.take(6, OPP, c, 1 - self.p.k)


def run_steps(unit, before, after):
    def step(i, _):
        for j, f in before.items():
            pl.when(i == j)(f)
        unit(i)
        for j, f in after.items():
            pl.when(i == j)(f)
        return 0

    lax.fori_loop(0, 8, step, 0)


def kernel(n, tok_ref, hot_ref, n1g, n1s, qkv_hbm, wo_hbm, ob_ref, n2g, n2s, up_hbm, ub_ref, down_hbm, db_ref, out_ref,
           res, buf, big, w_qk, w_v, w_up, w_down, qk_s, v_s, qm_s, km_s, hots, heads_s, got,
           hid, sibp, direct, midr, omid, msum, fin,
           w_sem, turn, h_ss, h_rs, ag_ss, ag_rs, wg_ss, wg_rs, mg_ss, mg_rs, a_ss, a_rs,
           d_ss, d_rs, s_ss, s_rs, m_ss, m_rs, o_ss, o_rs, f_ss, f_rs):
    p = Peers(n)
    k, me = p.k, p.me
    layers, _, heads, dim, dm = qkv_hbm.shape
    ff = w_up.shape[1]
    rows = 2 * HALF
    scale = dim ** -0.5 * LOG2E
    entry = pltpu.get_barrier_semaphore()
    p.greet(entry)

    def qkv_loads(l):
        out = []
        for t in range(2):
            for h in range(heads):
                out.append(pltpu.make_async_copy(qkv_hbm.at[l, t, h], w_qk.at[t * heads + h, 0:dim, :], w_sem.at[t * heads + h]))
        for h in range(heads):
            out.append(pltpu.make_async_copy(qkv_hbm.at[l, 2, h], w_v.at[pl.ds(h * dim, dim), :], w_sem.at[2 * heads + h]))
        return out

    def out_loads(l):
        return [pltpu.make_async_copy(wo_hbm.at[l, pl.ds(s * HALF, HALF), :], big.at[s, k], w_sem.at[3 * heads + s]) for s in range(2)]

    def mlp_loads(l):
        up = pltpu.make_async_copy(up_hbm.at[l], w_up, w_sem.at[3 * heads + 2])
        return [up, pltpu.make_async_copy(down_hbm.at[l], w_down, w_sem.at[3 * heads + 3])]

    for c in qkv_loads(0):
        c.start()
    for t in range(2 * heads):
        w_qk[t, dim:PAD, :] = jnp.zeros((PAD - dim, dm), BF16)
    hots[me] = hot_ref[...]

    def widen(c, _):
        r = pl.ds(pl.multiple_of(c * CH, CH), CH)
        res[r, :] = tok_ref[r, :].astype(F32)
        return 0

    lax.fori_loop(0, 4, widen, 0)

    def norm_rows(gain, shift):
        def part(c, _):
            x = res[pl.ds(pl.multiple_of(c * CH, CH), CH), :]
            cen = x - jnp.mean(x, axis=1, keepdims=True)
            var = jnp.mean(cen * cen, axis=1, keepdims=True)
            h = (cen * lax.rsqrt(var + 1e-5) * gain + shift).astype(BF16)
            buf[c // 2, k, pl.ds(pl.multiple_of((c % 2) * CH, CH), CH), :] = h
            return 0

        lax.fori_loop(0, 4, part, 0)

    docs = hot_ref.shape[0]
    lanes = lax.broadcasted_iota(jnp.int32, (QB, PAD), 1)
    row = lax.broadcasted_iota(jnp.int32, (QB, QB), 0)
    col = lax.broadcasted_iota(jnp.int32, (QB, QB), 1)
    low = lax.broadcasted_iota(jnp.int32, (1, PAD), 1) < dim

    def masks():
        for d in range(1, n):
            src = lax.rem(me + n - d, n)
            copy(hots.at[src], hots.at[src], h_ss.at[d - 1], h_rs.at[d - 1], p.sib).wait_recv()
        lane = lax.broadcasted_iota(jnp.int32, (docs, PAD), 1)
        place = lax.broadcasted_iota(jnp.int32, (docs, PAD), 0)
        pick = jnp.where(lane == place + dim, 1.0, 0.0).astype(BF16)
        used = jnp.where((lanes >= dim) & (lanes < dim + docs), 1.0, 0.0).astype(F32)

        def one(i, _):
            x = lax.dot_general(hots[i], pick, (((0,), (0,)), ((), ())), preferred_element_type=F32)
            r = pl.ds(pl.multiple_of(i * QB, QB), QB)
            qm_s[r, :] = (x * -8e30).astype(BF16)
            km_s[r, :] = (used - x).astype(BF16)
            return 0

        lax.fori_loop(0, n, one, 0)

    def layer(l, _):
        at_l = pl.ds(l, 1)
        for c in out_loads(l) + mlp_loads(l):
            c.start()
        norm_rows(n1g[at_l, :], n1s[at_l, :])

        @pl.when(l == 0)
        def _():
            p.met(entry)
            for d in range(1, n):
                copy(hot_ref, hots.at[me], h_ss.at[d - 1], h_rs.at[d - 1], {"tp": lax.rem(me + d, n)}).start()

        @pl.when(l > 0)
        def _():
            p.met(turn)

        g = Gather(p, buf, ag_ss, ag_rs)
        gw = WeightGather(p, big, wg_ss, wg_rs)
        for c in range(4):
            g.start(c)
        for c in qkv_loads(l):
            c.wait()
        pl.when(l == 0)(masks)

        def project_in(i):
            x = buf[i].reshape(rows, dm)
            middle = (i >= 2) & (i < 6)
            half = jnp.where(middle, i // 2 - 1, lax.rem(i, 2))
            chip = jnp.where(i < 2, p.chip, jnp.where(middle, jnp.where(lax.rem(i, 2) == 0, p.left, p.right), p.opp))
            spots = [pl.ds(pl.multiple_of((2 * chip + kk) * rows + half * HALF, HALF), HALF) for kk in range(2)]
            for t in range(2):
                w = w_qk[t * heads:(t + 1) * heads].reshape(heads * PAD, dm)
                y = lax.dot_general(x, w, (((1,), (1,)), ((), ())), preferred_element_type=F32)
                for kk in range(2):
                    mask = (qm_s if t == 0 else km_s)[spots[kk], :].astype(F32)
                    for h in range(heads):
                        part = y[kk * HALF:(kk + 1) * HALF, h * PAD:(h + 1) * PAD] + mask
                        qk_s[spots[kk], (t * heads + h) * PAD:(t * heads + h + 1) * PAD] = part.astype(BF16)
            y = lax.dot_general(x, w_v[...], (((1,), (1,)), ((), ())), preferred_element_type=F32).astype(BF16)
            for kk in range(2):
                v_s[spots[kk], :] = y[kk * HALF:(kk + 1) * HALF, :]

        def arrivals(gg):
            def four():
                gg.near_sibling(2)
                gg.near_sibling(3)

            def six():
                for c in (0, 1):
                    gg.far(c)
                for c in (0, 1):
                    gg.far_sibling(c)

            def seven():
                for c in (2, 3):
                    gg.far(c)
                for c in (2, 3):
                    gg.far_sibling(c)

            def zero():
                gg.sibling(0)
                gg.sibling(1)

            def one():
                gg.sibling(2)
                gg.sibling(3)

            def two():
                gg.near_sibling(0)
                gg.near_sibling(1)

            return {0: zero, 1: one, 2: two, 4: four, 6: six, 7: seven}

        def after_three():
            g.near(2)
            g.near(3)
            for c in out_loads(l):
                c.wait()
            gw.start()

        run_steps(project_in, arrivals(g), {0: lambda: g.near(0), 1: lambda: g.near(1), 3: after_three})
        g.drain()

        @pl.when(l + 1 < layers)
        def _():
            for c in qkv_loads(l + 1):
                c.start()

        diag = jnp.where(col <= row, 0.0, -8e30).astype(F32)

        def block(i):
            lo, hi = i * QB, (i + 1) * QB
            for gr in range(heads // 2):
                pair_v = v_s[0:hi, gr * PAD:(gr + 1) * PAD]
                zero = jnp.zeros_like(pair_v)
                out = None
                for b in range(2):
                    h = 2 * gr + b
                    q = qk_s[lo:hi, h * PAD:(h + 1) * PAD]
                    kk = qk_s[0:hi, (heads + h) * PAD:(heads + h + 1) * PAD]
                    s = lax.dot_general(q, kk, (((1,), (1,)), ((), ())), preferred_element_type=F32)
                    sd = s[:, lo:] + diag
                    s = jnp.concatenate([s[:, :lo], sd], axis=1) if i else sd
                    m = jnp.max(s, axis=1, keepdims=True)
                    e = jnp.exp2((s - m) * scale)
                    total = jnp.sum(e, axis=1, keepdims=True)
                    pr = (e * (1.0 / total)).astype(BF16)
                    v = jnp.where(low, pair_v, zero) if b == 0 else jnp.where(low, zero, pair_v)
                    o = jnp.dot(pr, v, preferred_element_type=F32)
                    out = o if out is None else out + o
                heads_s[i, :, gr * PAD:(gr + 1) * PAD] = out.astype(BF16)

        def to_owner(i):
            return copy(heads_s.at[i], got.at[me], a_ss.at[i], a_rs.at[me], {"tp": me * 0 + i})

        for i in range(n):
            block(i)

            @pl.when(me != i)
            def _():
                to_owner(i).start()

            if i == n - 6:
                gw.near(0)
            elif i == n - 5:
                gw.near(1)
            elif i == n - 4:
                gw.near(2)
            elif i == n - 3:
                gw.near(3)
                gw.near(4)
            elif i == n - 2:
                gw.twin_near(0)
                gw.twin_near(1)
        for i in range(3):
            gw.far(i)
        gw.twin_near(2)
        gw.sibling()
        got[me] = heads_s[me]
        DN = 512

        def project(o, chip, core, first=False):
            a = got[2 * chip + core]

            def tile(j, _):
                cols = pl.ds(pl.multiple_of(j * DN, DN), DN)
                w = jnp.concatenate([big[slot(o, 0), core, :, cols], big[slot(o, 1), core, :, cols]], axis=0)
                y = jnp.dot(a, w, preferred_element_type=F32).astype(BF16).astype(F32)
                if first:
                    y = y + ob_ref[at_l, cols]
                res[:, cols] += y
                return 0

            lax.fori_loop(0, dm // DN, tile, 0)

        def arrive(src):
            copy(got.at[src], got.at[src], a_ss.at[src], a_rs.at[src], p.sib).wait_recv()

        arrive(2 * p.chip + 1 - k)
        project(OWN, p.chip, 0, True)
        project(OWN, p.chip, 1)
        gw.far(3)
        gw.far(4)
        gw.near_sibling()
        for o, chip in ((LEFT, p.left), (RIGHT, p.right)):
            for kk in range(2):
                arrive(2 * chip + kk)
                project(o, chip, kk)
        for i in range(3):
            gw.twin_far(i)
        gw.far_sibling()
        for kk in range(2):
            arrive(2 * p.opp + kk)
            project(OPP, p.opp, kk)
        gw.drain()
        for i in range(n):
            @pl.when(me != i)
            def _():
                to_owner(i).wait_send()

        norm_rows(n2g[at_l, :], n2s[at_l, :])
        gm = Gather(p, buf, mg_ss, mg_rs)
        cp = Copies(p)
        for c in range(4):
            gm.start(c)
        for c in mlp_loads(l):
            c.wait()
        UN, DN = 512, 512

        def feed(i):
            def up(j, _):
                cols = pl.ds(pl.multiple_of(j * UN, UN), UN)
                a = jnp.dot(buf[i].reshape(rows, dm), w_up[:, cols], preferred_element_type=F32) + ub_ref[at_l, cols]
                cdf = 0.5 * (1.0 + jnp.tanh(0.7978845608028654 * (a + 0.044715 * (a * a * a))))
                hid[:, cols] = (a * cdf).astype(BF16)
                return 0

            def down(j, _):
                cols = pl.ds(pl.multiple_of(j * DN, DN), DN)
                y = jnp.dot(hid[...], w_down[:, cols], preferred_element_type=F32).astype(BF16)
                big[i, :, :, cols] = y.reshape(2, HALF, DN)
                return 0

            lax.fori_loop(0, ff // UN, up, 0)
            lax.fori_loop(0, dm // DN, down, 0)

        def send_direct(s):
            cp.send(lambda: copy(big.at[slot(RIGHT, s), 1], direct.at[k, s], d_ss.at[0, s], d_rs.at[k, s], p.to_right[1]))
            cp.send(lambda: copy(big.at[slot(LEFT, s), 0], direct.at[k, s], d_ss.at[1, s], d_rs.at[k, s], p.to_left[0]))

        def send_opposite(s):
            for j in range(2):
                r = pl.ds(j * CH, CH)
                cp.send(lambda j=j, r=r: copy(big.at[slot(OPP, s), 0, r, :], omid.at[0, k, r, :], o_ss.at[0, s, j], o_rs.at[0, k, j], p.to_right[s]))
                cp.send(lambda j=j, r=r: copy(big.at[slot(OPP, s), 1, r, :], omid.at[1, k, r, :], o_ss.at[1, s, j], o_rs.at[1, k, j], p.to_left[s]))

        def m_one():
            gm.near(1)
            for s in range(2):
                cp.send(lambda s=s: copy(big.at[s, 1 - k], sibp.at[s], s_ss.at[s], s_rs.at[s], p.sib))

        def m_three():
            gm.near(2)
            gm.near(3)
            send_direct(0)

        def m_five():
            send_direct(1)
            cp.send(lambda: copy(big.at[3 + 2 * (1 - k), 0], midr.at[0], m_ss.at[0], m_rs.at[0], p.sib))
            cp.send(lambda: copy(big.at[2 + 2 * (1 - k), 1], midr.at[1], m_ss.at[1], m_rs.at[1], p.sib))

        run_steps(feed, arrivals(gm), {0: lambda: gm.near(0), 1: m_one, 3: m_three, 5: m_five, 6: lambda: send_opposite(0), 7: lambda: send_opposite(1)})
        for e in range(2):
            cp.recv(midr.at[e], m_ss.at[e], m_rs.at[e])
        for j in range(2):
            r = pl.ds(j * CH, CH)
            for e in range(2):
                for q in range(2):
                    cp.recv(omid.at[e, q, r, :], o_ss.at[e, q, j], o_rs.at[e, q, j])
                own = big[(3 if e == 0 else 2) + 2 * k, e, r, :].astype(F32)
                msum[e, r, :] = (own + midr[e, r, :].astype(F32)) + (omid[e, 0, r, :].astype(F32) + omid[e, 1, r, :].astype(F32))
                cp.send(lambda e=e, j=j, r=r: copy(msum.at[e, r, :], fin.at[k, r, :], f_ss.at[e, j], f_rs.at[k, j], p.to_right[0] if e == 0 else p.to_left[1]))
        for s in range(2):
            cp.recv(sibp.at[s], s_ss.at[s], s_rs.at[s])
            for q in range(2):
                cp.recv(direct.at[q, s], d_ss.at[q, s], d_rs.at[q, s])
            o = pl.ds(s * HALF, HALF)
            near = (big[s, k].astype(F32) + sibp[s].astype(F32)) + (direct[0, s].astype(F32) + direct[1, s].astype(F32))
            res[o, :] += near + db_ref[at_l, :]
        for j in range(2):
            r = pl.ds(j * CH, CH)
            for s in range(2):
                cp.recv(fin.at[s, r, :], f_ss.at[s, j], f_rs.at[s, j])
                o = pl.ds(s * HALF + j * CH, CH)
                res[o, :] += fin[s, r, :]
        gm.drain()
        cp.drain()

        @pl.when(l + 1 < layers)
        def _():
            p.greet(turn)

        return 0

    lax.fori_loop(0, layers, layer, 0)
    for d in range(1, n):
        copy(hot_ref, hots.at[me], h_ss.at[d - 1], h_rs.at[d - 1], {"tp": lax.rem(me + d, n)}).wait_send()

    def narrow(c, _):
        r = pl.ds(pl.multiple_of(c * CH, CH), CH)
        out_ref[r, :] = res[r, :].astype(BF16)
        return 0

    lax.fori_loop(0, 4, narrow, 0)


def solution(mesh):
    n = mesh.shape["tp"]
    row_spec = P("dp", "tp", None)
    vec_spec = P(None, None)
    in_specs = (row_spec, P("dp", "tp"), vec_spec, vec_spec, P(None, None, None, "tp", None), P(None, "tp", None, None), vec_spec, vec_spec, vec_spec, P(None, None, "tp"), P(None, "tp"), P(None, "tp", None), vec_spec)

    def device_fn(tokens, doc_ids, norm1_gain, norm1_shift, qkv_weight, out_weight, out_bias, norm2_gain, norm2_shift, up_weight, up_bias, down_weight, down_bias):
        layers, dm, _, heads, dim = qkv_weight.shape
        rows = tokens.shape[1]
        seq = n * rows
        ff = up_weight.shape[2]
        hot = (jnp.arange(16, dtype=jnp.int32)[:, None] == doc_ids).astype(BF16)
        qkv_t = jnp.transpose(qkv_weight, (0, 2, 3, 4, 1))
        out_w = out_weight.reshape(layers, heads * dim, dm)

        def body(*refs):
            kernel(n, *refs)

        vm = pl.BlockSpec(memory_space=pltpu.VMEM)
        hb = pl.BlockSpec(memory_space=pl.ANY)
        dma = pltpu.SemaphoreType.DMA
        v = pltpu.VMEM
        out = pl.pallas_call(
            body,
            out_shape=jax.ShapeDtypeStruct((rows, dm), BF16),
            in_specs=[vm, vm, vm, vm, hb, hb, vm, vm, vm, hb, vm, hb, vm],
            out_specs=vm,
            scratch_shapes=[
                v((rows, dm), F32),
                v((8, 2, HALF, dm), BF16),
                v((8, 2, HALF, dm), BF16),
                v((2 * heads, PAD, dm), BF16),
                v((heads * dim, dm), BF16),
                v((dm, ff), BF16),
                v((ff, dm), BF16),
                v((seq, 2 * heads * PAD), BF16),
                v((seq, heads * dim), BF16),
                v((seq, PAD), BF16),
                v((seq, PAD), BF16),
                v((n,) + hot.shape, BF16),
                v((n, rows, heads * dim), BF16),
                v((n, rows, heads * dim), BF16),
                v((rows, ff), BF16),
                v((2, HALF, dm), BF16),
                v((2, 2, HALF, dm), BF16),
                v((2, HALF, dm), BF16),
                v((2, 2, HALF, dm), BF16),
                v((2, HALF, dm), F32),
                v((2, HALF, dm), F32),
                dma((3 * heads + 4,)), pltpu.SemaphoreType.REGULAR,
                dma((n - 1,)), dma((n - 1,)), dma((7, 4)), dma((7, 4)), dma((10, 8)), dma((10, 8)), dma((7, 4)), dma((7, 4)), dma((n,)), dma((n,)),
                dma((2, 2)), dma((2, 2)), dma((2,)), dma((2,)), dma((2,)), dma((2,)),
                dma((2, 2, 2)), dma((2, 2, 2)), dma((2, 2)), dma((2, 2)),
            ],
            name="gpt_layers",
            compiler_params=pltpu.CompilerParams(collective_id=3, has_side_effects=True, vmem_limit_bytes=67_043_328),
        )(tokens[0], hot, norm1_gain, norm1_shift, qkv_t, out_w, out_bias, norm2_gain, norm2_shift, up_weight, up_bias, down_weight, down_bias)
        return out[None]

    return jax.shard_map(device_fn, mesh=mesh, in_specs=in_specs, out_specs=row_spec, check_vma=False)
```
